32 devices in a mesh: group: 2 (over x), tile: 16 (over z, y, core).
Axes of the slice: x: 2, y: 2, z: 4, core: 2. Of those that a mesh axis runs over, the one named last changes fastest.
Arguments:
- hadamard: int32 [128, 1152], P(None, 'tile'), may hold values from -1 to 1, as said below
- stroke: float32 [2304], P(('group', 'tile')), parts along dimension 0, may hold values from 0.3 to 1
- influence: bfloat16 [3, 2304, 8192], P(None, ('group', 'tile')), parts along dimension 1, may hold values from -0.4375 to 0.4375
- amplitude: float32 [1024, 16, 16], P(('group', 'tile')), parts along dimension 0, may hold values from 0.3 to 1
- aberration: float32 [1024, 16, 16], P(('group', 'tile')), parts along dimension 0, may hold values from -3 to 3
- valid_mask: int32 [1024], P(('group', 'tile')), parts along dimension 0, may hold values from 0 to 1, as said below
Outputs:
- imat: float32 [2304, 2, 512], P(('group', 'tile')), parts along dimension 0
The draws below stay inside these ranges and needn't reach their ends.
There are 2 independent parts, one for each index of `group`. The reference program is written for one: setup_inputs(seed, part) draws one part's arguments, and reference() takes and returns one part's arrays. A program takes and returns all parts, laid end to end along the dimension named above; an argument that names none is the same for every part. Nothing has to cross between parts.
Inputs may be any that keep to these rules, and one draw needn't show every extreme that they name: `hadamard`: each column is one column of a Sylvester-Hadamard matrix whose order is the least power of two not below 1152, restricted to 128 distinct rows of it; different actuators take different columns. `valid_mask`: every pupil tile of 32 subapertures holds at least one valid subaperture.
All inputs are finite; a program needn't handle non-finite values.
Results may differ from the reference program's by a relative error of at most 0.0055.
Values may be sent and summed in bfloat16 or wider, within the bound.
A program may use at most 128 MiB of HBM per device.

```python
import math
import jax
import jax.numpy as jnp
from jax import lax

PAT = 128
ACT_DEV = 72
SUB_DEV = 32
SAMP = 16
PIX = 16
ACTS = 1152
SUBS = 512
PTS = 8192
N_TILE = 16


def draw_hadamard(key, part):
    order_bits = max(1, (ACTS - 1).bit_length())
    order = 2 ** order_bits
    row_pick = jax.random.permutation(jax.random.fold_in(key, 17), order)[:PAT].astype(jnp.int32)
    column_pick = jax.random.permutation(jax.random.fold_in(key, 29), order)[:ACTS].astype(jnp.int32)
    shared = jnp.bitwise_and(row_pick[:, None], column_pick[None, :])
    parity = jnp.zeros((PAT, ACTS), jnp.int32)
    for place in range(order_bits):
        parity = jnp.bitwise_xor(parity, jnp.bitwise_and(jnp.right_shift(shared, place), 1))
    return (1 - 2 * parity).astype(jnp.int32)


def draw_valid_mask(key, part):
    base_draw = jax.random.randint(jax.random.fold_in(key, 41), (N_TILE, SUB_DEV), 0, 4)
    base_mask = (base_draw < 3).astype(jnp.int32)
    forced_place = jax.random.randint(jax.random.fold_in(key, 53), (N_TILE, 1), 0, SUB_DEV)
    places = jnp.arange(SUB_DEV, dtype=jnp.int32)[None, :]
    forced = (places == forced_place).astype(jnp.int32)
    return jnp.maximum(base_mask, forced).reshape(SUBS).astype(jnp.int32)


def block_scale(stream_key, extent, shards, low, largest):
    factor_of, own = 1.0, jax.random.fold_in(stream_key, 6)
    for axis_at, shards_of in shards:
        draws = jnp.exp(jax.random.uniform(jax.random.fold_in(own, axis_at), (shards_of,), jnp.float32, low / len(shards), largest / len(shards)))
        factor_of = factor_of * jnp.repeat(draws, extent[axis_at] // shards_of).reshape([-1 if axis == axis_at else 1 for axis in range(len(extent))])
    return factor_of


def normal_values(own_key, dims, width, most, pieces=(), kind=jnp.bfloat16):
    level = block_scale(own_key, dims, pieces, -0.22, 0.18) if pieces else 1.0
    drawn = jax.random.normal(own_key, dims, jnp.float32) * width * level
    return jnp.minimum(jnp.maximum(drawn, -most), most).astype(kind)


def setup_inputs(seed: int = 0, part: int = 0) -> dict:
    splits = jax.random.split(jax.random.key(seed), 7)
    own_keys = jax.random.split(jax.random.fold_in(splits[6], part), 7)
    return {
        "hadamard": draw_hadamard(jax.random.fold_in(splits[6], 71), part),
        "stroke": jnp.clip(jnp.exp(math.log(1.0) - 1.2039728 * jax.random.uniform(own_keys[1], (ACTS,), jnp.float32) ** block_scale(own_keys[1], (ACTS,), ((0, 16),), -0.2, 0.2)), 0.3, 1.0),
        "influence": normal_values(own_keys[2], (3, ACTS, PTS), (3 * ACT_DEV) ** -0.5, 0.4375, ((1, 16),)),
        "amplitude": jnp.clip(jnp.exp(math.log(1.0) - 1.2039728 * jax.random.uniform(own_keys[3], (SUBS, SAMP, SAMP), jnp.float32) ** block_scale(own_keys[3], (SUBS, SAMP, SAMP), ((0, 16),), -0.2, 0.2)), 0.3, 1.0),
        "aberration": normal_values(own_keys[4], (SUBS, SAMP, SAMP), 0.5, 3.0, ((0, 16),), jnp.float32),
        "valid_mask": draw_valid_mask(jax.random.fold_in(jax.random.fold_in(splits[6], part), 71), part),
    }


HIGHEST = lax.Precision.HIGHEST


def transform_tables(samples, pixels):
    freqs = jnp.arange(pixels, dtype=jnp.float32) - pixels / 2.0
    places = jnp.arange(samples, dtype=jnp.float32)
    angle = 2.0 * jnp.pi * freqs[:, None] * places[None, :] / (2.0 * samples)
    return jnp.cos(angle), -jnp.sin(angle)


def kron_tables(samples, pixels):
    table_real, table_imag = transform_tables(samples, pixels)
    kron_real = jnp.kron(table_real, table_real) - jnp.kron(table_imag, table_imag)
    kron_imag = jnp.kron(table_real, table_imag) + jnp.kron(table_imag, table_real)
    upper = jnp.concatenate([kron_real.T, kron_imag.T], axis=1)
    lower = jnp.concatenate([-kron_imag.T, kron_real.T], axis=1)
    transform = jnp.concatenate([upper, lower], axis=0)
    centre = jnp.arange(pixels, dtype=jnp.float32) - (pixels - 1) / 2.0
    along_u = jnp.repeat(centre, pixels)
    along_v = jnp.tile(centre, pixels)
    moments = jnp.stack([jnp.ones_like(along_u), along_u, along_v], axis=1)
    return transform, moments


def spot_slopes(phase_map, amplitude, aberration, valid_mask):
    patterns, sub_count, samples = phase_map.shape[0], phase_map.shape[1], phase_map.shape[2]
    flat = samples * samples
    transform, moments = kron_tables(samples, PIX)
    half = PIX * PIX
    phase_rows = phase_map.reshape(patterns, sub_count, flat)
    amp_rows = amplitude.reshape(sub_count, flat)[None]
    abe_rows = aberration.reshape(sub_count, flat)[None]
    results = []
    for pattern_sign in (1.0, -1.0):
        angles = abe_rows + pattern_sign * phase_rows
        field = jnp.concatenate([amp_rows * jnp.cos(angles), amp_rows * jnp.sin(angles)], axis=2)
        focal = jnp.dot(field.reshape(patterns * sub_count, 2 * flat), transform, precision=HIGHEST)
        intensity = focal[:, :half] * focal[:, :half] + focal[:, half:] * focal[:, half:]
        sums = jnp.dot(intensity, moments, precision=HIGHEST)
        centroid_x = sums[:, 1] / sums[:, 0]
        centroid_y = sums[:, 2] / sums[:, 0]
        results.append(jnp.stack([centroid_x, centroid_y], axis=1).reshape(patterns, sub_count, 2).transpose(0, 2, 1))
    weights = valid_mask.astype(jnp.float32)[None, None, :]
    return ((results[0] - results[1]) * 0.5 * weights).astype(jnp.bfloat16)


def reference(hadamard, stroke, influence, amplitude, aberration, valid_mask):
    commands = (stroke[None, :] * hadamard.astype(jnp.float32)).astype(jnp.bfloat16)

    def one_tile(tile_index):
        phase_map = jnp.zeros((PAT, PTS), jnp.float32)
        for offset in range(3):
            source = tile_index + 1 - offset
            inside = (source >= 0) & (source < N_TILE)
            clipped = jnp.clip(source, 0, N_TILE - 1).astype(jnp.int32)
            block_cmds = lax.dynamic_slice_in_dim(commands, clipped * ACT_DEV, ACT_DEV, 1)
            block_infl = lax.dynamic_slice_in_dim(influence[offset], clipped * ACT_DEV, ACT_DEV, 0)
            term = jnp.dot(block_cmds, block_infl, preferred_element_type=jnp.float32).astype(jnp.bfloat16)
            term = lax.optimization_barrier(term).astype(jnp.float32)
            phase_map = phase_map + jnp.where(inside, term, jnp.zeros_like(term))
        first = (tile_index * SUB_DEV).astype(jnp.int32)
        amp_tile = lax.dynamic_slice_in_dim(amplitude, first, SUB_DEV, 0)
        abe_tile = lax.dynamic_slice_in_dim(aberration, first, SUB_DEV, 0)
        mask_tile = lax.dynamic_slice_in_dim(valid_mask, first, SUB_DEV, 0)
        return spot_slopes(phase_map.reshape(PAT, SUB_DEV, SAMP, SAMP), amp_tile, abe_tile, mask_tile)

    per_tile = lax.map(one_tile, jnp.arange(N_TILE, dtype=jnp.int32))
    slopes = jnp.transpose(per_tile, (1, 2, 0, 3)).reshape(PAT, 2 * SUBS)
    summed = jnp.dot(hadamard.astype(jnp.bfloat16).T, slopes, preferred_element_type=jnp.float32)
    return summed.reshape(ACTS, 2, SUBS) / (PAT * stroke)[:, None, None]
```

```python
import functools
import math

import jax
import jax.numpy as jnp
import numpy as np
from jax import lax
from jax.experimental import pallas as pl
from jax.experimental.pallas import tpu as pltpu
from jax.sharding import PartitionSpec as P

PIX = 16
MESH = pl.DeviceIdType.MESH
NT = (((1,), (1,)), ((), ()))


def dft_table(samples, pixels):
    freqs = np.arange(pixels) - pixels / 2.0
    wave = np.exp(-2j * np.pi * freqs[:, None] * np.arange(samples)[None, :] / (2.0 * samples))
    kron = np.kron(wave, wave)
    return np.block([[kron.real, -kron.imag], [kron.imag, kron.real]]).astype(np.float32)


def poly_fit(func, degree):
    fit = np.polynomial.chebyshev.Chebyshev.interpolate(func, degree, domain=[0.0, 0.25])
    return [float(c) for c in fit.convert(kind=np.polynomial.Polynomial).coef]


def sin_over_r(z):
    return 2 * np.pi * np.sinc(2 * np.sqrt(z))


COS = poly_fit(lambda z: np.cos(2 * np.pi * np.sqrt(z)), 5)
SIN = poly_fit(sin_over_r, 5)


def horner(coefs, z):
    total = coefs[-1] * z + coefs[-2]
    for c in coefs[-3::-1]:
        total = total * z + c
    return total


def cos_sin(phase):
    turns = phase * (1.0 / (2.0 * math.pi))
    r = turns - jnp.round(turns)
    z = r * r
    return horner(COS, z), r * horner(SIN, z)


def column_sums(planes):
    pix = len(planes)
    run = planes[-1]
    nested = run
    for plane in planes[-2::-1]:
        run = run + plane
        nested = nested + run
    places = lax.broadcasted_iota(jnp.int32, run.shape, 0).astype(jnp.float32)
    centre = (pix - 1) / 2.0
    along_u = nested - (centre + 1.0) * run
    along_v = run * (places - centre)
    return [jnp.sum(x, axis=0, keepdims=True) for x in (run, along_u, along_v)]


def spot_rows(phase, real, imag, table):
    patterns = phase.shape[0]
    cs, sn = cos_sin(phase)
    even = jnp.concatenate([(cs * real).astype(jnp.bfloat16), (cs * imag).astype(jnp.bfloat16)], axis=1)
    odd = jnp.concatenate([(sn * -imag).astype(jnp.bfloat16), (sn * real).astype(jnp.bfloat16)], axis=1)
    field = jnp.concatenate([even, odd], axis=0)
    focal = lax.dot_general(table, field, NT, preferred_element_type=jnp.float32)
    half = focal.shape[0] // 2
    squares, crosses = [], []
    for u in range(PIX):
        re = focal[u * PIX:(u + 1) * PIX]
        im = focal[half + u * PIX:half + (u + 1) * PIX]
        c_re, s_re = re[:, :patterns], re[:, patterns:]
        c_im, s_im = im[:, :patterns], im[:, patterns:]
        squares.append((c_re * c_re + c_im * c_im) + (s_re * s_re + s_im * s_im))
        crosses.append(c_re * s_re + c_im * s_im)
    p0, pu, pv = column_sums(squares)
    q0, qu, qv = [2.0 * x for x in column_sums(crosses)]
    scale = 1.0 / ((p0 + q0) * (p0 - q0))
    return (qu * p0 - pu * q0) * scale, (qv * p0 - pv * q0) * scale


def diagonal_column(row):
    k = row.shape[1]
    shape = (k, k)
    same = lax.broadcasted_iota(jnp.int32, shape, 0) == lax.broadcasted_iota(jnp.int32, shape, 1)
    return jnp.sum(jnp.where(same, jnp.broadcast_to(row, shape), 0.0), axis=1, keepdims=True)


def slopes_kernel(
    n, chunks, per, flat, parts,
    had_hbm, stroke_hbm, infl_ref, amp_hbm, abe_hbm, mask_hbm, table_hbm,
    held_ref,
    had, stroke, amp, abe, mask, table,
    mid_buf, low_buf, up_buf, cmds, cmds_low, cmds_up, real, imag, rows, mine,
    load_sems, mid_sems, send_sems, recv_sems, cmd_send, cmd_recv, own_sems, push_send, push_recv,
):
    me = lax.axis_index("tile")
    has_low, has_up = me > 0, me < n - 1
    low_id, up_id = {"tile": jnp.maximum(me - 1, 0)}, {"tile": jnp.minimum(me + 1, n - 1)}
    width = per * flat
    subs = mine.shape[1]
    part = subs // parts
    barrier = pltpu.get_barrier_semaphore()

    @pl.loop(1, n)
    def _(k):
        pl.semaphore_signal(barrier, inc=1, device_id={"tile": lax.rem(me + k, n)}, device_id_type=MESH)

    def columns(c):
        return pl.ds(pl.multiple_of(c * width, width), width)

    def mid_copy(c):
        return pltpu.make_async_copy(infl_ref.at[1, :, columns(c)], mid_buf.at[c], mid_sems.at[c])

    def remote(src, dst, send, recv, device):
        return pltpu.make_async_remote_copy(
            src_ref=src, dst_ref=dst, send_sem=send, recv_sem=recv, device_id=device, device_id_type=MESH
        )

    def to_up(c):
        return remote(infl_ref.at[2, :, columns(c)], low_buf.at[c], send_sems.at[0, c], recv_sems.at[0, c], up_id)

    def to_low(c):
        return remote(infl_ref.at[0, :, columns(c)], up_buf.at[c], send_sems.at[1, c], recv_sems.at[1, c], low_id)

    def cmds_to_up():
        return remote(cmds, cmds_low, cmd_send.at[0], cmd_recv.at[0], up_id)

    def cmds_to_low():
        return remote(cmds, cmds_up, cmd_send.at[1], cmd_recv.at[1], low_id)

    loads = [
        pltpu.make_async_copy(src, dst, load_sems.at[k])
        for k, (src, dst) in enumerate([
            (had_hbm, had), (stroke_hbm, stroke), (abe_hbm, abe), (amp_hbm, amp), (mask_hbm, mask), (table_hbm, table),
        ])
    ]
    for load in loads:
        load.start()

    @pl.loop(0, chunks)
    def _(c):
        mid_copy(c).start()

    loads[0].wait()
    loads[1].wait()
    cmds[...] = (had[...].astype(jnp.float32) * diagonal_column(stroke[...])).astype(jnp.bfloat16)

    pl.semaphore_wait(barrier, n - 1)

    @pl.when(has_up)
    def _():
        cmds_to_up().start()

    @pl.when(has_low)
    def _():
        cmds_to_low().start()

    @pl.loop(0, chunks)
    def _(c):
        @pl.when(has_up)
        def _():
            to_up(c).start()

        @pl.when(has_low)
        def _():
            to_low(c).start()

    @pl.when(jnp.logical_not(has_low))
    def _():
        cmds_low[...] = jnp.zeros_like(cmds_low)
        low_buf[...] = jnp.zeros_like(low_buf)

    @pl.when(jnp.logical_not(has_up))
    def _():
        cmds_up[...] = jnp.zeros_like(cmds_up)
        up_buf[...] = jnp.zeros_like(up_buf)

    for load in loads[2:]:
        load.wait()
    cs, sn = cos_sin(abe[...])
    whole_real, whole_imag = (amp[...] * cs).T, (amp[...] * sn).T
    for c in range(chunks):
        real[c] = whole_real[c * per:(c + 1) * per]
        imag[c] = whole_imag[c * per:(c + 1) * per]
    mask_column = diagonal_column(mask[...].astype(jnp.float32))

    @pl.when(has_up)
    def _():
        cmds_to_up().wait_send()
        cmds_to_low().wait_recv()

    @pl.when(has_low)
    def _():
        cmds_to_low().wait_send()
        cmds_to_up().wait_recv()

    mid_cmds = cmds[...].T
    low_cmds = cmds_low[...].T
    up_cmds = cmds_up[...].T

    def slot(g):
        return held_ref.at[:, pl.ds(pl.multiple_of(me * subs + g * part, part), part), :]

    def piece(g):
        return mine.at[:, pl.ds(g * part, part), :]

    def own(g):
        return pltpu.make_async_copy(piece(g), slot(g), own_sems.at[g])

    def push(g, k):
        return remote(piece(g), slot(g), push_send.at[g, k], push_recv.at[g, k], {"tile": lax.rem(me + k, n)})

    steps = chunks // parts
    for g in range(parts):
        @pl.loop(g * steps, (g + 1) * steps)
        def _(c):
            mid_copy(c).wait()

            @pl.when(has_low)
            def _():
                to_up(c).wait_recv()

            @pl.when(has_up)
            def _():
                to_low(c).wait_recv()

            rows_u, rows_v = [], []
            for k in range(per):
                cols = slice(k * flat, (k + 1) * flat)
                phase = jnp.dot(low_cmds, low_buf[c, :, cols], preferred_element_type=jnp.float32)
                phase += jnp.dot(mid_cmds, mid_buf[c, :, cols], preferred_element_type=jnp.float32)
                phase += jnp.dot(up_cmds, up_buf[c, :, cols], preferred_element_type=jnp.float32)
                along_u, along_v = spot_rows(phase, real[c, k:k + 1, :], imag[c, k:k + 1, :], table[...])
                rows_u.append(along_u)
                rows_v.append(along_v)
            rows[c, 0] = jnp.concatenate(rows_u, axis=0)
            rows[c, 1] = jnp.concatenate(rows_v, axis=0)

        for j in range(2):
            whole = jnp.concatenate([rows[c, j] for c in range(g * steps, (g + 1) * steps)], axis=0)
            mine[j, g * part:(g + 1) * part] = (whole * mask_column[g * part:(g + 1) * part]).astype(mine.dtype)
        own(g).start()

        @pl.loop(1, n)
        def _(k):
            push(g, k).start()

    @pl.loop(0, chunks)
    def _(c):
        @pl.when(has_up)
        def _():
            to_up(c).wait_send()

        @pl.when(has_low)
        def _():
            to_low(c).wait_send()

    for g in range(parts):
        own(g).wait()

        @pl.loop(1, n)
        def _(k):
            push(g, k).wait()


def apply_kernel(held, had_ref, stroke_ref, out_ref):
    patterns = had_ref.shape[1]
    signs = had_ref[...].astype(jnp.float32).astype(jnp.bfloat16)
    scale = patterns * diagonal_column(stroke_ref[...])
    for c in range(2):
        summed = lax.dot_general(signs, held[c], NT, preferred_element_type=jnp.float32)
        out_ref[:, c, :] = summed / scale


def per_device(hadamard, stroke, influence, amplitude, aberration, valid_mask):
    n = lax.axis_size("tile")
    patterns, acts = hadamard.shape
    subs, samples = amplitude.shape[0], amplitude.shape[1]
    flat = samples * samples
    per = math.gcd(subs, 2)
    chunks = subs // per
    parts = 2 if subs % 32 == 0 else 1
    had = hadamard.T
    amp = amplitude.transpose(1, 2, 0).reshape(flat, subs)
    abe = aberration.transpose(1, 2, 0).reshape(flat, subs)
    stroke = stroke.reshape(1, acts)
    mask = valid_mask.reshape(1, subs)
    table = jnp.asarray(dft_table(samples, PIX), dtype=jnp.bfloat16)
    vmem = pl.BlockSpec(memory_space=pltpu.VMEM)
    hbm = pl.BlockSpec(memory_space=pltpu.HBM)
    slab = pltpu.VMEM((chunks, acts, per * flat), jnp.bfloat16)
    held = pl.pallas_call(
        functools.partial(slopes_kernel, n, chunks, per, flat, parts),
        out_shape=jax.ShapeDtypeStruct((2, n * subs, patterns), jnp.bfloat16),
        in_specs=[hbm] * 7,
        out_specs=vmem,
        scratch_shapes=[
            pltpu.VMEM((acts, patterns), jnp.int32),
            pltpu.VMEM((1, acts), jnp.float32),
            pltpu.VMEM((flat, subs), jnp.float32),
            pltpu.VMEM((flat, subs), jnp.float32),
            pltpu.VMEM((1, subs), jnp.int32),
            pltpu.VMEM(table.shape, jnp.bfloat16),
            slab, slab, slab,
            pltpu.VMEM((acts, patterns), jnp.bfloat16),
            pltpu.VMEM((acts, patterns), jnp.bfloat16),
            pltpu.VMEM((acts, patterns), jnp.bfloat16),
            pltpu.VMEM((chunks, per, flat), jnp.float32),
            pltpu.VMEM((chunks, per, flat), jnp.float32),
            pltpu.VMEM((chunks, 2, per, patterns), jnp.float32),
            pltpu.VMEM((2, subs, patterns), jnp.bfloat16),
            pltpu.SemaphoreType.DMA((6,)),
            pltpu.SemaphoreType.DMA((chunks,)),
            pltpu.SemaphoreType.DMA((2, chunks)),
            pltpu.SemaphoreType.DMA((2, chunks)),
            pltpu.SemaphoreType.DMA((2,)),
            pltpu.SemaphoreType.DMA((2,)),
            pltpu.SemaphoreType.DMA((parts,)),
            pltpu.SemaphoreType.DMA((parts, n)),
            pltpu.SemaphoreType.DMA((parts, n)),
        ],
        compiler_params=pltpu.CompilerParams(
            collective_id=1, has_side_effects=True, vmem_limit_bytes=62 * 1024 * 1024
        ),
        name="slopes",
    )(had, stroke, influence, amp, abe, mask, table)
    return pl.pallas_call(
        apply_kernel,
        out_shape=jax.ShapeDtypeStruct((acts, 2, n * subs), jnp.float32),
        in_specs=[vmem] * 3,
        out_specs=vmem,
        name="apply",
    )(held, had, stroke)


def solution(mesh):
    placed = (
        P(None, "tile"),
        P(("group", "tile")),
        P(None, ("group", "tile"), None),
        P(("group", "tile"), None, None),
        P(("group", "tile"), None, None),
        P(("group", "tile")),
    )
    return jax.shard_map(
        per_device,
        mesh=mesh,
        in_specs=placed,
        out_specs=P(("group", "tile"), None, None),
        check_vma=False,
    )
```

```python
import functools
import math

import jax
import jax.numpy as jnp
import numpy as np
from jax import lax
from jax.experimental import pallas as pl
from jax.experimental.pallas import tpu as pltpu
from jax.sharding import PartitionSpec as P

PIX = 16
NEAR = 4
FAR = 6
AHEAD = 3
BIAS = 8
MESH = pl.DeviceIdType.MESH
NT = (((1,), (1,)), ((), ()))


def dft_table(samples, pixels):
    freqs = np.arange(pixels) - pixels / 2.0
    wave = np.exp(-2j * np.pi * freqs[:, None] * np.arange(samples)[None, :] / (2.0 * samples))
    kron = np.kron(wave, wave)
    return np.block([[kron.real, -kron.imag], [kron.imag, kron.real]]).astype(np.float32)


def poly_fit(func, degree):
    fit = np.polynomial.chebyshev.Chebyshev.interpolate(func, degree, domain=[0.0, 0.25])
    return [float(c) for c in fit.convert(kind=np.polynomial.Polynomial).coef]


def sin_over_r(z):
    return 2 * np.pi * np.sinc(2 * np.sqrt(z))


COS = poly_fit(lambda z: np.cos(2 * np.pi * np.sqrt(z)), 5)
SIN = poly_fit(sin_over_r, 5)


def horner(coefs, z):
    total = coefs[-1] * z + coefs[-2]
    for c in coefs[-3::-1]:
        total = total * z + c
    return total


def cos_sin(phase):
    turns = phase * (1.0 / (2.0 * math.pi))
    r = turns - jnp.round(turns)
    z = r * r
    return horner(COS, z), r * horner(SIN, z)


def column_sums(planes):
    pix = len(planes)
    run = planes[-1]
    nested = run
    for plane in planes[-2::-1]:
        run = run + plane
        nested = nested + run
    places = lax.broadcasted_iota(jnp.int32, run.shape, 0).astype(jnp.float32)
    centre = (pix - 1) / 2.0
    along_u = nested - (centre + 1.0) * run
    along_v = run * (places - centre)
    return [jnp.sum(x, axis=0, keepdims=True) for x in (run, along_u, along_v)]


def spot_rows(phase, real, imag, table):
    patterns = phase.shape[0]
    cs, sn = cos_sin(phase)
    even = jnp.concatenate([(cs * real).astype(jnp.bfloat16), (cs * imag).astype(jnp.bfloat16)], axis=1)
    odd = jnp.concatenate([(sn * -imag).astype(jnp.bfloat16), (sn * real).astype(jnp.bfloat16)], axis=1)
    field = jnp.concatenate([even, odd], axis=0)
    focal = lax.dot_general(table, field, NT, preferred_element_type=jnp.float32)
    half = focal.shape[0] // 2
    squares, crosses = [], []
    for u in range(PIX):
        re = focal[u * PIX:(u + 1) * PIX]
        im = focal[half + u * PIX:half + (u + 1) * PIX]
        c_re, s_re = re[:, :patterns], re[:, patterns:]
        c_im, s_im = im[:, :patterns], im[:, patterns:]
        squares.append((c_re * c_re + c_im * c_im) + (s_re * s_re + s_im * s_im))
        crosses.append(c_re * s_re + c_im * s_im)
    p0, pu, pv = column_sums(squares)
    q0, qu, qv = [2.0 * x for x in column_sums(crosses)]
    scale = 1.0 / ((p0 + q0) * (p0 - q0))
    return (qu * p0 - pu * q0) * scale, (qv * p0 - pv * q0) * scale


def diagonal_column(row):
    k = row.shape[1]
    shape = (k, k)
    same = lax.broadcasted_iota(jnp.int32, shape, 0) == lax.broadcasted_iota(jnp.int32, shape, 1)
    return jnp.sum(jnp.where(same, jnp.broadcast_to(row, shape), 0.0), axis=1, keepdims=True)


def slopes_kernel(
    n, relays, chunks, per, flat, parts,
    had_hbm, stroke_hbm, infl_ref, amp_hbm, abe_hbm, mask_hbm, table_hbm,
    held_ref,
    had, stroke, amp, abe, mask, table,
    mid_buf, low_buf, up_buf, cmds, cmds_low, cmds_up, real, imag, rows, mask_rows, mine, passing,
    load_sems, mid_sems, send_sems, recv_sems, cmd_send, cmd_recv, own_sems, push_send, push_recv, known, pass_send, pass_recv,
):
    me = lax.axis_index("tile")
    has_low, has_up = me > 0, me < n - 1
    low_id, up_id = {"tile": jnp.maximum(me - 1, 0)}, {"tile": jnp.minimum(me + 1, n - 1)}
    width = per * flat
    part = mine.shape[2]
    subs = parts * part
    steps = chunks // parts
    rounds = (n - 1).bit_length()
    span_up = jnp.where(lax.rem(me, 4) == 3, FAR, NEAR)
    span_low = jnp.where(lax.rem(me, 4) == 0, FAR, NEAR)
    barrier = pltpu.get_barrier_semaphore()

    def greet(sem, distance):
        @pl.when(me >= distance)
        def _():
            pl.semaphore_signal(sem, inc=1, device_id={"tile": me - distance}, device_id_type=MESH)

        @pl.when(me < n - distance)
        def _():
            pl.semaphore_signal(sem, inc=1, device_id={"tile": me + distance}, device_id_type=MESH)

    def met(sem, distance):
        both = jnp.logical_and(me >= distance, me < n - distance)
        either = jnp.logical_or(me >= distance, me < n - distance)

        @pl.when(both)
        def _():
            pl.semaphore_wait(sem, 2)

        @pl.when(jnp.logical_and(either, jnp.logical_not(both)))
        def _():
            pl.semaphore_wait(sem, 1)

    place = lax.rem(me, 4)
    levels = n // 4
    far_up = jnp.logical_and(place == 3, has_up)
    far_low = jnp.logical_and(place == 0, has_low)
    pass_up = jnp.logical_and(place == 1, me + 3 < n)
    pass_low = jnp.logical_and(place == 2, me >= 3)

    def salute(condition, offset):
        @pl.when(condition)
        def _():
            pl.semaphore_signal(barrier, inc=1, device_id={"tile": me + offset}, device_id_type=MESH)

    greet(barrier, 1)
    if relays:
        for condition, offsets in ((far_up, (-2, 3)), (far_low, (2, -3)), (pass_up, (2, 3)), (pass_low, (-2, -3))):
            for offset in offsets:
                salute(condition, offset)

    def columns(c):
        return pl.ds(pl.multiple_of(c * width, width), width)

    def mid_copy(c):
        return pltpu.make_async_copy(infl_ref.at[1, :, columns(c)], mid_buf.at[c], mid_sems.at[c])

    def remote(src, dst, send, recv, device):
        return pltpu.make_async_remote_copy(
            src_ref=src, dst_ref=dst, send_sem=send, recv_sem=recv, device_id=device, device_id_type=MESH
        )

    def detour(level, c, count_up):
        low = chunks * (level + 1) // levels - chunks // BIAS
        count = chunks - low if count_up else low
        return ((c + 1) * count) // chunks != (c * count) // chunks

    def via_up(t, c):
        return detour(t // 4, c, True)

    def via_low(t, c):
        return detour(t // 4 - 1, c, False)

    def aside_up(c):
        source = infl_ref.at[2, :, columns(c)]
        return remote(source, passing.at[c], send_sems.at[0, c], pass_recv.at[c], {"tile": jnp.maximum(me - 2, 0)})

    def aside_low(c):
        source = infl_ref.at[0, :, columns(c)]
        return remote(source, passing.at[c], send_sems.at[1, c], pass_recv.at[c], {"tile": jnp.minimum(me + 2, n - 1)})

    def onward_up(c):
        target = {"tile": jnp.minimum(me + 3, n - 1)}
        return remote(passing.at[c], low_buf.at[c], pass_send.at[c], recv_sems.at[0, c], target)

    def onward_low(c):
        target = {"tile": jnp.maximum(me - 3, 0)}
        return remote(passing.at[c], up_buf.at[c], pass_send.at[c], recv_sems.at[1, c], target)

    def relay(c):
        @pl.when(jnp.logical_and(pass_up, via_up(me + 2, c)))
        def _():
            aside_up(c).wait_recv()
            onward_up(c).start()

        @pl.when(jnp.logical_and(pass_low, via_low(me - 2, c)))
        def _():
            aside_low(c).wait_recv()
            onward_low(c).start()

    def relay_done(c):
        @pl.when(jnp.logical_and(pass_up, via_up(me + 2, c)))
        def _():
            onward_up(c).wait_send()

        @pl.when(jnp.logical_and(pass_low, via_low(me - 2, c)))
        def _():
            onward_low(c).wait_send()

    def to_up(c):
        return remote(infl_ref.at[2, :, columns(c)], low_buf.at[c], send_sems.at[0, c], recv_sems.at[0, c], up_id)

    def to_low(c):
        return remote(infl_ref.at[0, :, columns(c)], up_buf.at[c], send_sems.at[1, c], recv_sems.at[1, c], low_id)

    def cmds_to_up():
        return remote(cmds, cmds_low, cmd_send.at[0], cmd_recv.at[0], up_id)

    def cmds_to_low():
        return remote(cmds, cmds_up, cmd_send.at[1], cmd_recv.at[1], low_id)

    loads = [
        pltpu.make_async_copy(src, dst, load_sems.at[k])
        for k, (src, dst) in enumerate([
            (had_hbm, had), (stroke_hbm, stroke), (abe_hbm, abe), (amp_hbm, amp), (mask_hbm, mask), (table_hbm, table),
        ])
    ]
    for load in loads:
        load.start()

    peers = has_low.astype(jnp.int32) + has_up.astype(jnp.int32)
    if relays:
        for condition in (far_up, far_low, pass_up, pass_low):
            peers += 2 * condition.astype(jnp.int32)
    pl.semaphore_wait(barrier, peers)

    def send_to(exists, far, span, c, straight, aside, via):
        m = c + span
        go = jnp.logical_and(exists, jnp.logical_and(m >= 0, m < chunks))
        around = jnp.logical_and(far, via(me, m)) if relays else False

        @pl.when(jnp.logical_and(go, jnp.logical_not(around)))
        def _():
            straight(m).start()

        if relays:
            @pl.when(jnp.logical_and(go, around))
            def _():
                aside(m).start()

    def send_slab(c):
        send_to(has_up, far_up, span_up, c, to_up, aside_up, via_up)
        send_to(has_low, far_low, span_low, c, to_low, aside_low, via_low)

    first = -max(NEAR, FAR)

    @pl.loop(first, first + 2)
    def _(c):
        send_slab(c)

    greet(known.at[0], 1)
    loads[0].wait()
    loads[1].wait()
    cmds[...] = (had[...].astype(jnp.float32) * diagonal_column(stroke[...])).astype(jnp.bfloat16)

    @pl.when(has_up)
    def _():
        cmds_to_up().start()

    @pl.when(has_low)
    def _():
        cmds_to_low().start()

    @pl.loop(first + 2, 0)
    def _(c):
        send_slab(c)

    @pl.loop(0, chunks)
    def _(c):
        mid_copy(c).start()

    @pl.when(jnp.logical_not(has_low))
    def _():
        cmds_low[...] = jnp.zeros_like(cmds_low)
        low_buf[...] = jnp.zeros_like(low_buf)

    @pl.when(jnp.logical_not(has_up))
    def _():
        cmds_up[...] = jnp.zeros_like(cmds_up)
        up_buf[...] = jnp.zeros_like(up_buf)

    for load in loads[2:]:
        load.wait()
    cs, sn = cos_sin(abe[...])
    whole_real, whole_imag = (amp[...] * cs).T, (amp[...] * sn).T
    for c in range(chunks):
        real[c] = whole_real[c * per:(c + 1) * per]
        imag[c] = whole_imag[c * per:(c + 1) * per]
    mask_column = diagonal_column(mask[...].astype(jnp.float32))
    for g in range(parts):
        mask_rows[g] = jnp.broadcast_to(mask_column[g * part:(g + 1) * part], mask_rows.shape[1:])

    @pl.when(has_up)
    def _():
        cmds_to_up().wait_send()
        cmds_to_low().wait_recv()

    @pl.when(has_low)
    def _():
        cmds_to_low().wait_send()
        cmds_to_up().wait_recv()

    if relays:
        @pl.loop(0, AHEAD)
        def _(c):
            relay(c)

    mid_cmds = cmds[...].T
    low_cmds = cmds_low[...].T
    up_cmds = cmds_up[...].T

    def slot(g):
        return held_ref.at[:, pl.ds(pl.multiple_of(me * subs + g * part, part), part), :]

    def own(g):
        return pltpu.make_async_copy(mine.at[g], slot(g), own_sems.at[g])

    def push(g, k):
        return remote(mine.at[g], slot(g), push_send.at[g, k], push_recv.at[g, k], {"tile": lax.rem(me + k, n)})

    @pl.loop(0, chunks)
    def _(c):
        mid_copy(c).wait()

        @pl.when(has_low)
        def _():
            to_up(c).wait_recv()

        @pl.when(has_up)
        def _():
            to_low(c).wait_recv()

        send_slab(c)
        if relays:
            @pl.when(c + AHEAD < chunks)
            def _():
                relay(c + AHEAD)

        rows_u, rows_v = [], []
        for k in range(per):
            cols = slice(k * flat, (k + 1) * flat)
            phase = jnp.dot(low_cmds, low_buf[c, :, cols], preferred_element_type=jnp.float32)
            phase += jnp.dot(mid_cmds, mid_buf[c, :, cols], preferred_element_type=jnp.float32)
            phase += jnp.dot(up_cmds, up_buf[c, :, cols], preferred_element_type=jnp.float32)
            along_u, along_v = spot_rows(phase, real[c, k:k + 1, :], imag[c, k:k + 1, :], table[...])
            rows_u.append(along_u)
            rows_v.append(along_v)
        rows[c, 0] = jnp.concatenate(rows_u, axis=0)
        rows[c, 1] = jnp.concatenate(rows_v, axis=0)

        for r in range(rounds):
            @pl.when(c == r * steps // rounds)
            def _():
                met(known.at[r], 2 ** r)
                if r + 1 < rounds:
                    greet(known.at[r + 1], 2 ** (r + 1))

        @pl.when(lax.rem(c, steps) == steps - 1)
        def _():
            g = c // steps
            for j in range(2):
                whole = jnp.concatenate([rows[g * steps + i, j] for i in range(steps)], axis=0)
                mine[g, j] = (whole * mask_rows[g]).astype(mine.dtype)
            own(g).start()

            @pl.loop(1, n)
            def _(k):
                push(g, k).start()

    @pl.loop(0, chunks)
    def _(c):
        @pl.when(has_up)
        def _():
            to_up(c).wait_send()

        @pl.when(has_low)
        def _():
            to_low(c).wait_send()

        if relays:
            relay_done(c)

    @pl.loop(0, parts)
    def _(g):
        own(g).wait()

        @pl.loop(1, n)
        def _(k):
            push(g, k).wait()


def apply_kernel(held, had_ref, stroke_ref, out_ref):
    patterns = had_ref.shape[1]
    signs = had_ref[...].astype(jnp.float32).astype(jnp.bfloat16)
    scale = patterns * diagonal_column(stroke_ref[...])
    for c in range(2):
        summed = lax.dot_general(signs, held[c], NT, preferred_element_type=jnp.float32)
        out_ref[:, c, :] = summed / scale


def per_device(relays, hadamard, stroke, influence, amplitude, aberration, valid_mask):
    n = lax.axis_size("tile")
    patterns, acts = hadamard.shape
    subs, samples = amplitude.shape[0], amplitude.shape[1]
    flat = samples * samples
    per = math.gcd(subs, 2)
    chunks = subs // per
    parts = subs // 8 if subs % 8 == 0 else 1
    had = hadamard.T
    amp = amplitude.transpose(1, 2, 0).reshape(flat, subs)
    abe = aberration.transpose(1, 2, 0).reshape(flat, subs)
    stroke = stroke.reshape(1, acts)
    mask = valid_mask.reshape(1, subs)
    table = jnp.asarray(dft_table(samples, PIX), dtype=jnp.bfloat16)
    vmem = pl.BlockSpec(memory_space=pltpu.VMEM)
    hbm = pl.BlockSpec(memory_space=pltpu.HBM)
    slab = pltpu.VMEM((chunks, acts, per * flat), jnp.bfloat16)
    held = pl.pallas_call(
        functools.partial(slopes_kernel, n, relays, chunks, per, flat, parts),
        out_shape=jax.ShapeDtypeStruct((2, n * subs, patterns), jnp.bfloat16),
        in_specs=[hbm] * 7,
        out_specs=hbm,
        scratch_shapes=[
            pltpu.VMEM((acts, patterns), jnp.int32),
            pltpu.VMEM((1, acts), jnp.float32),
            pltpu.VMEM((flat, subs), jnp.float32),
            pltpu.VMEM((flat, subs), jnp.float32),
            pltpu.VMEM((1, subs), jnp.int32),
            pltpu.VMEM(table.shape, jnp.bfloat16),
            slab, slab, slab,
            pltpu.VMEM((acts, patterns), jnp.bfloat16),
            pltpu.VMEM((acts, patterns), jnp.bfloat16),
            pltpu.VMEM((acts, patterns), jnp.bfloat16),
            pltpu.VMEM((chunks, per, flat), jnp.float32),
            pltpu.VMEM((chunks, per, flat), jnp.float32),
            pltpu.VMEM((chunks, 2, per, patterns), jnp.float32),
            pltpu.VMEM((parts, subs // parts, patterns), jnp.float32),
            pltpu.VMEM((parts, 2, subs // parts, patterns), jnp.bfloat16),
            slab if relays else pltpu.VMEM((8, 128), jnp.bfloat16),
            pltpu.SemaphoreType.DMA((6,)),
            pltpu.SemaphoreType.DMA((chunks,)),
            pltpu.SemaphoreType.DMA((2, chunks)),
            pltpu.SemaphoreType.DMA((2, chunks)),
            pltpu.SemaphoreType.DMA((2,)),
            pltpu.SemaphoreType.DMA((2,)),
            pltpu.SemaphoreType.DMA((parts,)),
            pltpu.SemaphoreType.DMA((parts, n)),
            pltpu.SemaphoreType.DMA((parts, n)),
            pltpu.SemaphoreType.REGULAR(((n - 1).bit_length(),)),
            pltpu.SemaphoreType.DMA((chunks,)),
            pltpu.SemaphoreType.DMA((chunks,)),
        ],
        compiler_params=pltpu.CompilerParams(
            collective_id=1, has_side_effects=True, vmem_limit_bytes=62 * 1024 * 1024
        ),
        name="slopes",
    )(had, stroke, influence, amp, abe, mask, table)
    return pl.pallas_call(
        apply_kernel,
        out_shape=jax.ShapeDtypeStruct((acts, 2, n * subs), jnp.float32),
        in_specs=[vmem] * 3,
        out_specs=vmem,
        name="apply",
    )(held, had, stroke)


def hops(mesh, a, b):
    first, second = (getattr(mesh.devices[0, t], "coords", None) for t in (a, b))
    if first is None or second is None:
        return 0
    return sum(abs(p - q) for p, q in zip(first, second))


def relays_fit(mesh):
    n = mesh.shape["tile"]
    if mesh.axis_names != ("group", "tile") or n % 4 or n < 8:
        return False
    for t in range(3, n - 1, 4):
        path = [(t, t + 1, 2), (t, t - 2, 1), (t - 2, t + 1, 1), (t + 1, t + 3, 1), (t + 3, t, 1)]
        if any(hops(mesh, a, b) != count for a, b, count in path):
            return False
    return True


def solution(mesh):
    placed = (
        P(None, "tile"),
        P(("group", "tile")),
        P(None, ("group", "tile"), None),
        P(("group", "tile"), None, None),
        P(("group", "tile"), None, None),
        P(("group", "tile")),
    )
    return jax.shard_map(
        functools.partial(per_device, relays_fit(mesh)),
        mesh=mesh,
        in_specs=placed,
        out_specs=P(("group", "tile"), None, None),
        check_vma=False,
    )
```

```python
import functools
import math

import jax
import jax.numpy as jnp
import numpy as np
from jax import lax
from jax.experimental import pallas as pl
from jax.experimental.pallas import tpu as pltpu
from jax.sharding import PartitionSpec as P

PIX = 16
CHIP = 4
NEAR = 4
FAR = 6
ASIDE = 6
AHEAD = 3
LATER = 3
MESH = pl.DeviceIdType.MESH
NT = (((1,), (1,)), ((), ()))


def dft_table(samples, pixels):
    freqs = np.arange(pixels) - pixels / 2.0
    wave = np.exp(-2j * np.pi * freqs[:, None] * np.arange(samples)[None, :] / (2.0 * samples))
    kron = np.kron(wave, wave)
    return np.stack([kron.real, kron.imag]).astype(np.float32)


def poly_fit(func, degree):
    fit = np.polynomial.chebyshev.Chebyshev.interpolate(func, degree, domain=[0.0, 0.25])
    return [float(c) for c in fit.convert(kind=np.polynomial.Polynomial).coef]


def sin_over_r(z):
    return 2 * np.pi * np.sinc(2 * np.sqrt(z))


COS = poly_fit(lambda z: np.cos(2 * np.pi * np.sqrt(z)), 5)
SIN = poly_fit(sin_over_r, 5)


def horner(coefs, z):
    total = coefs[-1] * z + coefs[-2]
    for c in coefs[-3::-1]:
        total = total * z + c
    return total


def cos_sin(phase):
    turns = phase * (1.0 / (2.0 * math.pi))
    r = turns - jnp.round(turns)
    z = r * r
    return horner(COS, z), r * horner(SIN, z)


def column_sums(planes):
    pix = len(planes)
    run = planes[-1]
    nested = run
    for plane in planes[-2::-1]:
        run = run + plane
        nested = nested + run
    places = lax.broadcasted_iota(jnp.int32, run.shape, 0).astype(jnp.float32)
    centre = (pix - 1) / 2.0
    along_u = nested - (centre + 1.0) * run
    along_v = run * (places - centre)
    return [jnp.sum(x, axis=0, keepdims=True) for x in (run, along_u, along_v)]


def spot_rows(transform, field):
    patterns = field.shape[0] // 2
    focal = lax.dot_general(transform, field, NT, preferred_element_type=jnp.float32)
    half = focal.shape[0] // 2
    squares, crosses = [], []
    for u in range(PIX):
        re = focal[u * PIX:(u + 1) * PIX]
        im = focal[half + u * PIX:half + (u + 1) * PIX]
        c_re, s_re = re[:, :patterns], re[:, patterns:]
        c_im, s_im = im[:, :patterns], im[:, patterns:]
        squares.append((c_re * c_re + c_im * c_im) + (s_re * s_re + s_im * s_im))
        crosses.append(c_im * s_re - c_re * s_im)
    p0, pu, pv = column_sums(squares)
    q0, qu, qv = [2.0 * x for x in column_sums(crosses)]
    scale = 1.0 / ((p0 + q0) * (p0 - q0))
    return (qu * p0 - pu * q0) * scale, (qv * p0 - pv * q0) * scale


def diagonal_column(row):
    k = row.shape[1]
    shape = (k, k)
    same = lax.broadcasted_iota(jnp.int32, shape, 0) == lax.broadcasted_iota(jnp.int32, shape, 1)
    return jnp.sum(jnp.where(same, jnp.broadcast_to(row, shape), 0.0), axis=1, keepdims=True)


def slopes_kernel(
    n, relays, chunks, per, flat, pieces,
    had_hbm, stroke_hbm, infl_ref, amp_hbm, abe_hbm, mask_hbm, table_hbm,
    held_ref,
    had, stroke, amp, abe, mask, table,
    slabs, cmds, cmds_all, real, imag, transforms, fields, rows, mask_rows, mine, passing,
    load_sems, mid_sems, send_sems, recv_sems, cmd_send, cmd_recv, own_sems, push_send, push_recv, known, pass_send, pass_recv, forward_send,
):
    me = lax.axis_index("tile")
    has_low, has_up = me > 0, me < n - 1
    low_id, up_id = {"tile": jnp.maximum(me - 1, 0)}, {"tile": jnp.minimum(me + 1, n - 1)}
    width = per * flat
    acts = cmds.shape[0]
    groups, quad = mine.shape[0], mine.shape[1] // 2
    subs = groups * quad
    steps = quad // per
    rounds = (n - 1).bit_length()
    barrier = pltpu.get_barrier_semaphore()

    def greet(sem, distance):
        @pl.when(me >= distance)
        def _():
            pl.semaphore_signal(sem, inc=1, device_id={"tile": me - distance}, device_id_type=MESH)

        @pl.when(me < n - distance)
        def _():
            pl.semaphore_signal(sem, inc=1, device_id={"tile": me + distance}, device_id_type=MESH)

    def met(sem, distance):
        both = jnp.logical_and(me >= distance, me < n - distance)
        either = jnp.logical_or(me >= distance, me < n - distance)

        @pl.when(both)
        def _():
            pl.semaphore_wait(sem, 2)

        @pl.when(jnp.logical_and(either, jnp.logical_not(both)))
        def _():
            pl.semaphore_wait(sem, 1)

    place = lax.rem(me, 4)
    levels = n // 4
    mirror = me + 2 - lax.rem(me, 4) // 2 * 4
    far_up = jnp.logical_and(place == 3, has_up)
    far_low = jnp.logical_and(place == 0, has_low)
    pass_up = jnp.logical_and(place == 1, me + 3 < n)
    pass_low = jnp.logical_and(place == 2, me >= 3)

    def salute(condition, offset):
        @pl.when(condition)
        def _():
            pl.semaphore_signal(barrier, inc=1, device_id={"tile": me + offset}, device_id_type=MESH)

    greet(barrier, 1)
    if relays:
        for condition, offsets in ((far_up, (-2, 3)), (far_low, (2, -3)), (pass_up, (2, 3)), (pass_low, (-2, -3))):
            for offset in offsets:
                salute(condition, offset)

    def columns(c):
        return pl.ds(pl.multiple_of(c * width, width), width)

    def mid_copy(c):
        return pltpu.make_async_copy(infl_ref.at[1, :, columns(c)], slabs.at[c, 1, :acts, :], mid_sems.at[c])

    def remote(src, dst, send, recv, device):
        return pltpu.make_async_remote_copy(
            src_ref=src, dst_ref=dst, send_sem=send, recv_sem=recv, device_id=device, device_id_type=MESH
        )

    def picked(c, count):
        return ((c + 1) * count) // chunks != (c * count) // chunks

    def via_up(t, c):
        return picked(c, chunks * (levels - t // 4 - 1) // levels + chunks // 8)

    def via_low(t, c):
        return picked(c, chunks * (t // 4) // levels)

    def aside_up(c):
        source = infl_ref.at[2, :, columns(c)]
        return remote(source, passing.at[c], send_sems.at[0, c], pass_recv.at[c], {"tile": jnp.maximum(me - 2, 0)})

    def aside_low(c):
        source = infl_ref.at[0, :, columns(c)]
        return remote(source, passing.at[c], send_sems.at[1, c], pass_recv.at[c], {"tile": jnp.minimum(me + 2, n - 1)})

    def onward_up(c):
        target = {"tile": jnp.minimum(me + 3, n - 1)}
        return remote(passing.at[c], slabs.at[c, 0, :acts, :], pass_send.at[c], recv_sems.at[0, c], target)

    def onward_low(c):
        target = {"tile": jnp.maximum(me - 3, 0)}
        return remote(passing.at[c], slabs.at[c, 2, :acts, :], pass_send.at[c], recv_sems.at[1, c], target)

    def relay(c):
        @pl.when(jnp.logical_and(pass_up, via_up(me + 2, c)))
        def _():
            aside_up(c).wait_recv()
            onward_up(c).start()

        @pl.when(jnp.logical_and(pass_low, via_low(me - 2, c)))
        def _():
            aside_low(c).wait_recv()
            onward_low(c).start()

    def relay_done(c):
        @pl.when(jnp.logical_and(pass_up, via_up(me + 2, c)))
        def _():
            onward_up(c).wait_send()

        @pl.when(jnp.logical_and(pass_low, via_low(me - 2, c)))
        def _():
            onward_low(c).wait_send()

    def to_up(c):
        return remote(infl_ref.at[2, :, columns(c)], slabs.at[c, 0, :acts, :], send_sems.at[0, c], recv_sems.at[0, c], up_id)

    def to_low(c):
        return remote(infl_ref.at[0, :, columns(c)], slabs.at[c, 2, :acts, :], send_sems.at[1, c], recv_sems.at[1, c], low_id)

    def cmds_to_up():
        return remote(cmds, cmds_all.at[0, :acts, :], cmd_send.at[0], cmd_recv.at[0], up_id)

    def cmds_to_low():
        return remote(cmds, cmds_all.at[2, :acts, :], cmd_send.at[1], cmd_recv.at[1], low_id)

    loads = [
        pltpu.make_async_copy(src, dst, load_sems.at[k])
        for k, (src, dst) in enumerate([
            (had_hbm, had), (stroke_hbm, stroke), (abe_hbm, abe), (amp_hbm, amp), (mask_hbm, mask), (table_hbm, table),
        ])
    ]
    for load in loads:
        load.start()

    peers = has_low.astype(jnp.int32) + has_up.astype(jnp.int32)
    if relays:
        for condition in (far_up, far_low, pass_up, pass_low):
            peers += 2 * condition.astype(jnp.int32)
    pl.semaphore_wait(barrier, peers)

    def send_to(exists, chip, far, c, straight, aside, via):
        def when(condition, m, copy):
            @pl.when(jnp.logical_and(condition, jnp.logical_and(m >= 0, m < chunks)))
            def _():
                copy(m).start()

        when(chip, c + CHIP, straight)
        when(jnp.logical_and(exists, jnp.logical_not(jnp.logical_or(chip, far))), c + NEAR, straight)
        if relays:
            when(jnp.logical_and(far, jnp.logical_not(via(me, c + FAR))), c + FAR, straight)
            when(jnp.logical_and(far, via(me, c + ASIDE)), c + ASIDE, aside)
        else:
            when(far, c + FAR, straight)

    def send_slab(c):
        send_to(has_up, lax.rem(me, 2) == 0, far_up, c, to_up, aside_up, via_up)
        send_to(has_low, lax.rem(me, 2) == 1, far_low, c, to_low, aside_low, via_low)

    first = -max(CHIP, NEAR, FAR, ASIDE)

    @pl.loop(first, first + 2)
    def _(c):
        send_slab(c)

    greet(known.at[0], 1)
    loads[0].wait()
    loads[1].wait()
    cmds[...] = (had[...].astype(jnp.float32) * diagonal_column(stroke[...])).astype(jnp.bfloat16)

    @pl.when(has_up)
    def _():
        cmds_to_up().start()

    @pl.when(has_low)
    def _():
        cmds_to_low().start()

    @pl.loop(first + 2, 0)
    def _(c):
        send_slab(c)

    @pl.loop(0, chunks)
    def _(c):
        mid_copy(c).start()

    pad = slabs.shape[2] - acts
    cmds_all[1, :acts] = cmds[...]
    for o in range(3):
        if pad:
            cmds_all[o, acts:] = jnp.zeros((pad, cmds_all.shape[2]), jnp.bfloat16)
            slabs[:, o, acts:] = jnp.zeros((chunks, pad, width), jnp.bfloat16)

    for absent, o in ((jnp.logical_not(has_low), 0), (jnp.logical_not(has_up), 2)):
        @pl.when(absent)
        def _():
            cmds_all[o] = jnp.zeros(cmds_all.shape[1:], jnp.bfloat16)

            @pl.loop(0, chunks)
            def _(c):
                slabs[c, o] = jnp.zeros(slabs.shape[2:], jnp.bfloat16)

    for load in loads[2:]:
        load.wait()
    cs, sn = cos_sin(abe[...])
    real[...] = (amp[...] * cs).T.reshape(real.shape)
    imag[...] = (amp[...] * sn).T.reshape(imag.shape)

    @pl.loop(0, subs)
    def _(k):
        re, im = real[k], imag[k]
        half = table.shape[1]
        transforms[k, :half] = (table[0] * re - table[1] * im).astype(jnp.bfloat16)
        transforms[k, half:] = (table[0] * im + table[1] * re).astype(jnp.bfloat16)

    mask_column = diagonal_column(mask[...].astype(jnp.float32))
    for g in range(groups):
        column_of = mask_column[g * quad:(g + 1) * quad]
        mask_rows[g] = jnp.broadcast_to(jnp.concatenate([column_of, column_of], axis=0), mask_rows.shape[1:])

    @pl.when(has_up)
    def _():
        cmds_to_up().wait_send()
        cmds_to_low().wait_recv()

    @pl.when(has_low)
    def _():
        cmds_to_low().wait_send()
        cmds_to_up().wait_recv()

    if relays:
        @pl.loop(0, AHEAD)
        def _(c):
            relay(c)

    all_cmds = cmds_all[...].reshape(3 * slabs.shape[2], cmds.shape[1]).T

    def slot(p, t):
        start, size = pieces[p]
        return held_ref.at[pl.ds(t * groups + start, size)]

    def piece(p):
        start, size = pieces[p]
        return mine.at[pl.ds(start, size)]

    def own(p):
        return pltpu.make_async_copy(piece(p), slot(p, me), own_sems.at[p])

    def push(p, t):
        return remote(piece(p), slot(p, me), push_send.at[p, t], push_recv.at[p, me], {"tile": t})

    def forward(p, t):
        return remote(slot(p, mirror), slot(p, mirror), forward_send.at[p, t], push_recv.at[p, mirror], {"tile": t})

    def landing(p, t):
        return remote(piece(p), slot(p, t), push_send.at[p, t], push_recv.at[p, t], {"tile": t})

    def mirrored(p):
        return relays and p == 0 and len(pieces) > 2

    def everyone(act):
        @pl.loop(1, n)
        def _(k):
            act(lax.rem(me + k, n))

    def column(act):
        @pl.loop(1, n // 2)
        def _(k):
            at = lax.rem(me // 4 * 2 + lax.rem(me, 2) + k, n // 2)
            act(at // 2 * 4 + lax.rem(me, 4) // 2 * 2 + lax.rem(at, 2))

    def spread(p, act):
        if mirrored(p):
            column(lambda t: act(push(p, t)))
            act(push(p, mirror))
        else:
            everyone(lambda t: act(push(p, t)))

    def arrive(c):
        mid_copy(c).wait()

        @pl.when(has_low)
        def _():
            to_up(c).wait_recv()

        @pl.when(has_up)
        def _():
            to_low(c).wait_recv()

        send_slab(c)
        if relays:
            @pl.when(c + AHEAD < chunks)
            def _():
                relay(c + AHEAD)

    def wavefront(c):
        for k in range(per):
            block = slabs[c, :, :, k * flat:(k + 1) * flat].reshape(all_cmds.shape[1], flat)
            cs, sn = cos_sin(jnp.dot(all_cmds, block, preferred_element_type=jnp.float32))
            half = cs.shape[0]
            fields[lax.rem(c, 2), k, :half] = cs.astype(jnp.bfloat16)
            fields[lax.rem(c, 2), k, half:] = sn.astype(jnp.bfloat16)

    def spots(c):
        rows_u, rows_v = [], []
        for k in range(per):
            along_u, along_v = spot_rows(transforms[c * per + k], fields[lax.rem(c, 2), k])
            rows_u.append(along_u)
            rows_v.append(along_v)
        rows[c, 0] = jnp.concatenate(rows_u, axis=0)
        rows[c, 1] = jnp.concatenate(rows_v, axis=0)

    def finish(c):
        for r in range(rounds):
            @pl.when(c == r)
            def _():
                met(known.at[r], 2 ** r)
                if r + 1 < rounds:
                    greet(known.at[r + 1], 2 ** (r + 1))

        @pl.when(lax.rem(c, steps) == steps - 1)
        def _():
            g = c // steps
            both = [rows[g * steps + i, j] for j in range(2) for i in range(steps)]
            mine[g] = (jnp.concatenate(both, axis=0) * mask_rows[g]).astype(mine.dtype)

        for p, (start, size) in enumerate(pieces):
            end = (start + size) * steps - 1

            @pl.when(c == end)
            def _():
                own(p).start()
                spread(p, lambda copy: copy.start())

            if mirrored(p):
                @pl.when(c == end + LATER)
                def _():
                    landing(p, mirror).wait_recv()
                    column(lambda t: forward(p, t).start())

    arrive(0)
    wavefront(0)

    @pl.loop(1, chunks)
    def _(c):
        arrive(c)
        spots(c - 1)
        wavefront(c)
        finish(c - 1)

    spots(chunks - 1)
    finish(chunks - 1)

    @pl.loop(0, chunks)
    def _(c):
        @pl.when(has_up)
        def _():
            to_up(c).wait_send()

        @pl.when(has_low)
        def _():
            to_low(c).wait_send()

        if relays:
            relay_done(c)

    for p in range(len(pieces)):
        own(p).wait()
        spread(p, lambda copy: copy.wait_send())
        if mirrored(p):
            column(lambda t: forward(p, t).wait_send())

        def landed(t):
            if mirrored(p):
                @pl.when(t != mirror)
                def _():
                    landing(p, t).wait_recv()
            else:
                landing(p, t).wait_recv()

        everyone(landed)


def apply_kernel(held, had_ref, stroke_ref, out_ref):
    patterns = had_ref.shape[1]
    blocks, height = held.shape[0], held.shape[1]
    signs = had_ref[...].astype(jnp.float32).astype(jnp.bfloat16)
    scale = patterns * diagonal_column(stroke_ref[...])
    pairs = held[...].astype(jnp.float32).reshape(blocks // 2, 2, height, patterns)
    first, second = pairs[:, 0], pairs[:, 1]
    upper = lax.broadcasted_iota(jnp.int32, first.shape, 1) < height // 2
    along_u = jnp.where(upper, first, pltpu.roll(second, height // 2, 1))
    along_v = jnp.where(upper, pltpu.roll(first, height // 2, 1), second)
    for c, along in enumerate((along_u, along_v)):
        slopes = along.reshape(blocks * height // 2, patterns).astype(jnp.bfloat16)
        summed = lax.dot_general(signs, slopes, NT, preferred_element_type=jnp.float32)
        out_ref[:, c, :] = summed / scale


def per_device(relays, hadamard, stroke, influence, amplitude, aberration, valid_mask):
    n = lax.axis_size("tile")
    patterns, acts = hadamard.shape
    subs, samples = amplitude.shape[0], amplitude.shape[1]
    flat = samples * samples
    per = math.gcd(subs, 2)
    chunks = subs // per
    groups = subs // 4
    bounds = [0, groups - 3, groups - 1, groups] if groups > 4 else [0, groups]
    pieces = tuple((a, b - a) for a, b in zip(bounds, bounds[1:]))
    parts = len(pieces)
    had = hadamard.T
    amp = amplitude.transpose(1, 2, 0).reshape(flat, subs)
    abe = aberration.transpose(1, 2, 0).reshape(flat, subs)
    stroke = stroke.reshape(1, acts)
    mask = valid_mask.reshape(1, subs)
    table = jnp.asarray(dft_table(samples, PIX), dtype=jnp.float32)
    depth = -(-acts // 16) * 16
    vmem = pl.BlockSpec(memory_space=pltpu.VMEM)
    hbm = pl.BlockSpec(memory_space=pltpu.HBM)
    slab = pltpu.VMEM((chunks, acts, per * flat), jnp.bfloat16)
    held = pl.pallas_call(
        functools.partial(slopes_kernel, n, relays, chunks, per, flat, pieces),
        out_shape=jax.ShapeDtypeStruct((n * groups, 8, patterns), jnp.bfloat16),
        in_specs=[hbm] * 7,
        out_specs=vmem,
        scratch_shapes=[
            pltpu.VMEM((acts, patterns), jnp.int32),
            pltpu.VMEM((1, acts), jnp.float32),
            pltpu.VMEM((flat, subs), jnp.float32),
            pltpu.VMEM((flat, subs), jnp.float32),
            pltpu.VMEM((1, subs), jnp.int32),
            pltpu.VMEM(table.shape, jnp.float32),
            pltpu.VMEM((chunks, 3, depth, per * flat), jnp.bfloat16),
            pltpu.VMEM((acts, patterns), jnp.bfloat16),
            pltpu.VMEM((3, depth, patterns), jnp.bfloat16),
            pltpu.VMEM((subs, 1, flat), jnp.float32),
            pltpu.VMEM((subs, 1, flat), jnp.float32),
            pltpu.VMEM((subs, 2 * PIX * PIX, flat), jnp.bfloat16),
            pltpu.VMEM((2, per, 2 * patterns, flat), jnp.bfloat16),
            pltpu.VMEM((chunks, 2, per, patterns), jnp.float32),
            pltpu.VMEM((groups, 8, patterns), jnp.float32),
            pltpu.VMEM((groups, 8, patterns), jnp.bfloat16),
            slab if relays else pltpu.VMEM((8, 128), jnp.bfloat16),
            pltpu.SemaphoreType.DMA((6,)),
            pltpu.SemaphoreType.DMA((chunks,)),
            pltpu.SemaphoreType.DMA((2, chunks)),
            pltpu.SemaphoreType.DMA((2, chunks)),
            pltpu.SemaphoreType.DMA((2,)),
            pltpu.SemaphoreType.DMA((2,)),
            pltpu.SemaphoreType.DMA((parts,)),
            pltpu.SemaphoreType.DMA((parts, n)),
            pltpu.SemaphoreType.DMA((parts, n)),
            pltpu.SemaphoreType.REGULAR(((n - 1).bit_length(),)),
            pltpu.SemaphoreType.DMA((chunks,)),
            pltpu.SemaphoreType.DMA((chunks,)),
            pltpu.SemaphoreType.DMA((parts, n)),
        ],
        compiler_params=pltpu.CompilerParams(
            collective_id=1, has_side_effects=True, vmem_limit_bytes=40 * 1024 * 1024
        ),
        name="slopes",
    )(*(pltpu.with_memory_space_constraint(x, pltpu.HBM) for x in (had, stroke, influence, amp, abe, mask, table)))
    return pl.pallas_call(
        apply_kernel,
        out_shape=jax.ShapeDtypeStruct((acts, 2, n * subs), jnp.float32),
        in_specs=[vmem] * 3,
        out_specs=vmem,
        compiler_params=pltpu.CompilerParams(vmem_limit_bytes=24 * 1024 * 1024),
        name="apply",
    )(held, had, stroke)


def hops(mesh, a, b):
    first, second = (getattr(mesh.devices[0, t], "coords", None) for t in (a, b))
    if first is None or second is None:
        return 0
    return sum(abs(p - q) for p, q in zip(first, second))


def relays_fit(mesh):
    n = mesh.shape["tile"]
    if mesh.axis_names != ("group", "tile") or n % 4 or n < 8:
        return False
    for t in range(3, n - 1, 4):
        path = [(t, t + 1, 2), (t, t - 2, 1), (t - 2, t + 1, 1), (t + 1, t + 3, 1), (t + 3, t, 1)]
        if any(hops(mesh, a, b) != count for a, b, count in path):
            return False
    return True


def solution(mesh):
    placed = (
        P(None, "tile"),
        P(("group", "tile")),
        P(None, ("group", "tile"), None),
        P(("group", "tile"), None, None),
        P(("group", "tile"), None, None),
        P(("group", "tile")),
    )
    return jax.shard_map(
        functools.partial(per_device, relays_fit(mesh)),
        mesh=mesh,
        in_specs=placed,
        out_specs=P(("group", "tile"), None, None),
        check_vma=False,
    )
```
